32 devices in a mesh: along: 8 (over z, x), cross: 4 (over y, core).
Axes of the slice: x: 2, y: 2, z: 4, core: 2. Of those that a mesh axis runs over, the one named last changes fastest.
Arguments:
- offsets: float32 [2, 32, 64, 128], P(None, 'along', 'cross'), may hold values from 0 to 1
- velocity: float32 [2, 32, 64, 128], P(None, 'along', 'cross'), may hold values from -6 to 6
- particle_mass: float32 [32, 64, 128], P('along', 'cross'), may hold values from 0.5 to 2
- neighbours: int32 [32, 64, 9], P('along', 'cross'), may hold values from -1 to 8, as said below
- owner_device: int32 [8, 4, 8192, 1], P('along', 'cross'), may hold values from 0 to 31; in each aligned block of 8192 rows (0 to 8191, 8192 to 16383, ..., all dimensions but the last counted through in order) at most 768 rows name the same one
- target_cell: int32 [8, 4, 8192], P('along', 'cross'), may hold values from 0 to 65535
- surface: float32 [3, 1024, 2048], P(None, 'along', 'cross'), may hold values from -6 to 6
- water_depth: float32 [1024, 2048], P('along', 'cross'), may hold values from 0.5 to 2
Outputs:
- grid_state: float32 [3, 1024, 2048], P(None, 'along', 'cross')
- density: float32 [32, 64, 128], P('along', 'cross')
- feedback: float32 [3, 32, 64, 128], P(None, 'along', 'cross')
The draws below stay inside these ranges and needn't reach their ends.
Inputs may be any that keep to these rules, and one draw needn't show every extreme that they name: `owner_device`: in the rows of one device, at most 768 particles name one owner device (numbered as along index times 4 plus cross index), a bound that some block reaches. `neighbours`: slot 0 holds 4, the tile itself; the other slots hold distinct window positions or -1 for padding.
All inputs are finite; a program needn't handle non-finite values.
Results may differ from the reference program's by a relative error of at most 0.0003.
Values sent between devices are 32-bit elements; how exact they have to be, the bound alone decides.
No kernel may reach another device: no remote copies, remote signals or barrier semaphores. Data moves between devices by JAX's collectives and lax.ppermute only.
A program may use at most 64 MiB of HBM per device.

```python
import math
import jax
import jax.numpy as jnp
import numpy as np
from jax import lax

TILE = 128
TA = 4
TC = 16
GA = 128
GC = 512
SUBSTEPS = 4
PART_DEV = 8192
CAP = 768
NTA = 32
NTC = 64
NA = 1024
NC = 2048
N_ALONG = 8
N_CROSS = 4
DEVICES = 32


def draw_neighbours(key, part):
    shape_tiles = (NTA, NTC)
    key_order, key_drop = jax.random.split(jax.random.fold_in(key, 7))
    scores = jax.random.randint(key_order, shape_tiles + (8,), 0, 1 << 20) * 8 + jnp.arange(8, dtype=jnp.int32)
    ranking = jnp.argsort(scores, axis=-1, stable=True)
    others = jnp.array([0, 1, 2, 3, 5, 6, 7, 8], jnp.int32)
    chosen = others[ranking]
    dropped = jax.random.randint(key_drop, shape_tiles + (8,), 0, 3) == 0
    chosen = jnp.where(dropped, -1, chosen)
    own_tile = jnp.full(shape_tiles + (1,), 4, jnp.int32)
    return jnp.concatenate([own_tile, chosen], axis=-1).astype(jnp.int32)


def touch_ends(entries, key, smallest, largest):
    longest = entries.shape.index(max(entries.shape))
    spots = []
    for shift in (0, 1):
        where = [jax.random.randint(jax.random.fold_in(key, axis), (), 0, length) for axis, length in enumerate(entries.shape)]
        where[longest] = (where[longest] + shift) % entries.shape[longest]
        spots.append(tuple(where))
    return entries.at[spots[0]].set(smallest).at[spots[1]].set(largest)


def shard_levels(key, dims, shards, smallest, top_value):
    def one(dim, blocks):
        draws = jax.random.uniform(jax.random.fold_in(jax.random.fold_in(key, 6), dim), (blocks,), jnp.float32, smallest / len(shards), top_value / len(shards))
        return jnp.repeat(jnp.exp(draws), dims[dim] // blocks).reshape((-1,) + (1,) * (len(dims) - dim - 1))

    factor_of = one(*shards[0])
    for cut in shards[1:]:
        factor_of = factor_of * one(*cut)
    return factor_of


def shared_out(key, own, number, rows, amount, top, bound, slope):
    order = jax.random.permutation(key, amount)
    crowded, usual = load_shares(amount, rows * top, bound, slope, True), load_shares(amount, rows * top, bound, slope, False)
    places = jnp.arange(amount)

    def named(sizes, turn):
        used = int((sizes > 0).sum())
        fixed = max(1, used // 4)
        passed = fixed + (places - fixed + turn * (used - fixed)) % max(1, amount - fixed)
        return jnp.zeros((amount,), jnp.int32).at[order[jnp.where(places < fixed, places, passed)]].set(jnp.asarray(sizes, jnp.int32))

    sizes = jnp.where(number % 4 == 0, named(crowded, number // 4), named(usual, number - number // 4 - 1))
    mixed = jax.random.permutation(jax.random.fold_in(own, 3), amount)
    source_of, receiver = mixed[0:amount // 2 * 2:2], mixed[1:amount // 2 * 2:2]
    slack = jnp.minimum(sizes[source_of] - 1, bound - sizes[receiver]) // 2
    slack = jnp.where((source_of == order[0]) | (receiver == order[0]) | (sizes[receiver] == 0), 0, jnp.maximum(slack, 0))
    passed = jax.random.randint(jax.random.fold_in(own, 4), (amount // 2,), 0, 1 << 20) % (slack + 1)
    sizes = sizes.at[source_of].add(-passed).at[receiver].add(passed)
    labels = jnp.searchsorted(jnp.cumsum(sizes), jnp.arange(rows * top), side="right").astype(jnp.int32)
    grid = labels.reshape(top, rows).T
    grid = grid[jax.random.permutation(jax.random.fold_in(own, 1), rows)]
    turn = jax.random.randint(jax.random.fold_in(own, 2), (rows, 1), 0, top)
    return jnp.take_along_axis(grid, (jnp.arange(top)[None, :] + turn) % top, axis=1)


def load_shares(amount, total, bound, lean, full):
    portions = [(1 << 20) // math.isqrt(standing ** lean) + 1 for standing in range(1, amount + 1)]
    largest = bound if full else min(bound, max(-(-total // amount), total * portions[0] // sum(portions)))
    least = 1 if total - largest >= amount - 1 else 0
    holding, rest = [largest] + [least] * (amount - 1), total - largest - least * (amount - 1)
    while rest > 0:
        candidates = [i for i in range(1, amount) if holding[i] < largest] or [i for i in range(1, amount) if holding[i] < bound]
        mass, budget = sum([portions[i] for i in candidates]), rest
        for i in candidates:
            more = min(bound - holding[i], max(1, budget * portions[i] // mass), rest)
            holding[i] = holding[i] + more
            rest = rest - more
    return np.array(holding)


def noise(key, extent, spread, most, pieces=(), kind=jnp.bfloat16):
    result = spread * jax.random.normal(key, extent, jnp.float32)
    if pieces:
        result = result * shard_levels(key, extent, pieces, -0.22, 0.18)
    return jnp.clip(result, -most, most).astype(kind)


def setup_inputs(seed: int = 0) -> dict:
    seeds = jax.random.split(jax.random.key(seed), 9)
    offsets = jnp.clip(1.0 * jax.random.uniform(seeds[0], (2, NTA, NTC, TILE), jnp.float32) ** shard_levels(seeds[0], (2, NTA, NTC, TILE), ((1, 8), (2, 4)), -0.2, 0.2), 0.0, 1.0)
    velocity = noise(seeds[1], (2, NTA, NTC, TILE), 1.0, 6.0, ((1, 8), (2, 4)), jnp.float32)
    particle_mass = jnp.clip(jnp.exp(math.log(2.0) - 1.3862944 * jax.random.uniform(seeds[2], (NTA, NTC, TILE), jnp.float32) ** shard_levels(seeds[2], (NTA, NTC, TILE), ((0, 8), (1, 4)), -0.2, 0.2)), 0.5, 2.0)
    neighbours = draw_neighbours(jax.random.fold_in(seeds[8], 71), 0)
    owner_device_keys = jax.random.split(jax.random.fold_in(seeds[4], 1), N_ALONG * N_CROSS * PART_DEV // PART_DEV)
    owner_device_turns = jax.random.permutation(jax.random.fold_in(seeds[4], 3), N_ALONG * N_CROSS * PART_DEV // PART_DEV)
    owner_device = jax.vmap(lambda own, number: shared_out(jax.random.fold_in(seeds[4], 2), own, number, PART_DEV, DEVICES, 1, CAP, 2))(owner_device_keys, owner_device_turns).reshape((N_ALONG, N_CROSS, PART_DEV, 1))
    target_cell = touch_ends(jax.random.randint(seeds[5], (N_ALONG, N_CROSS, PART_DEV), 0, GA * GC), jax.random.fold_in(seeds[5], 1), 0, (GA * GC) - 1).astype(jnp.int32)
    surface = noise(seeds[6], (3, NA, NC), 1.0, 6.0, ((1, 8), (2, 4)), jnp.float32)
    water_depth = jnp.clip(jnp.exp(math.log(2.0) - 1.3862944 * jax.random.uniform(seeds[7], (NA, NC), jnp.float32) ** shard_levels(seeds[7], (NA, NC), ((0, 8), (1, 4)), -0.2, 0.2)), 0.5, 2.0)
    return {"offsets": offsets, "velocity": velocity, "particle_mass": particle_mass, "neighbours": neighbours, "owner_device": owner_device, "target_cell": target_cell, "surface": surface, "water_depth": water_depth}


courant = 0.4
kernel_width = 1.0


def tile_sums(window_rows, present_row):
    columns = window_rows.shape[2] - 2
    own_row = window_rows[:, 1, 1:columns + 1, :]
    totals = jnp.zeros((3, columns, window_rows.shape[3]), jnp.float32)
    for window in range(9):
        row_shift = window // 3
        col_shift = window % 3
        nearby = window_rows[:, row_shift, col_shift:col_shift + columns, :]
        delta_x = own_row[0][:, :, None] - nearby[0][:, None, :] - (row_shift - 1.0)
        delta_y = own_row[1][:, :, None] - nearby[1][:, None, :] - (col_shift - 1.0)
        weights = jnp.exp(-(delta_x * delta_x + delta_y * delta_y) / kernel_width)
        weights = weights * present_row[:, window][:, None, None]
        carried = jnp.stack([nearby[4], nearby[4] * nearby[2], nearby[4] * nearby[3]])
        totals = totals + jnp.einsum("tab,ktb->kta", weights, carried, precision=lax.Precision.HIGHEST)
    return totals


def particle_pass(padded, neighbours):
    rows = padded.shape[1] - 2
    present = jnp.any(neighbours[..., :, None] == jnp.arange(9, dtype=jnp.int32), axis=-2).astype(jnp.float32)

    def one_row(row_index):
        window_rows = lax.dynamic_slice_in_dim(padded, row_index, 3, 1)
        present_row = lax.dynamic_index_in_dim(present, row_index, 0, keepdims=False)
        return tile_sums(window_rows, present_row)

    totals = lax.map(one_row, jnp.arange(rows, dtype=jnp.int32))
    return jnp.transpose(totals, (1, 0, 2, 3))


def particle_sources(totals, particle_mass, tile_size):
    density = totals[0] / tile_size
    volume = particle_mass / density
    smooth_x = totals[1] / totals[0]
    smooth_y = totals[2] / totals[0]
    return density, jnp.stack([volume, volume * smooth_x, volume * smooth_y])


def lax_friedrichs(state_pad, depth_pad):
    height = state_pad[0]
    speed_x = state_pad[1]
    speed_y = state_pad[2]
    flux_x = depth_pad * speed_x
    flux_y = depth_pad * speed_y

    def average(quantity):
        return 0.25 * (quantity[2:, 1:-1] + quantity[:-2, 1:-1] + quantity[1:-1, 2:] + quantity[1:-1, :-2])

    next_height = average(height) - 0.5 * courant * (flux_x[2:, 1:-1] - flux_x[:-2, 1:-1] + flux_y[1:-1, 2:] - flux_y[1:-1, :-2])
    next_speed_x = average(speed_x) - 0.5 * courant * (height[2:, 1:-1] - height[:-2, 1:-1])
    next_speed_y = average(speed_y) - 0.5 * courant * (height[1:-1, 2:] - height[1:-1, :-2])
    return jnp.stack([next_height, next_speed_x, next_speed_y])


def reference(offsets, velocity, particle_mass, neighbours, owner_device, target_cell, surface, water_depth):
    stacked = jnp.concatenate([offsets, velocity, particle_mass[None]], axis=0)
    padded = jnp.pad(stacked, ((0, 0), (1, 1), (1, 1), (0, 0)))
    totals = particle_pass(padded, neighbours)
    density, sources = particle_sources(totals, particle_mass, TILE)
    ordered = sources.reshape(3, N_ALONG, TA, N_CROSS, TC, TILE).transpose(0, 1, 3, 2, 4, 5).reshape(3, -1)
    owners = owner_device.reshape(-1)
    cells = target_cell.reshape(-1)
    grid_row = (owners // N_CROSS) * GA + cells // GC
    grid_col = (owners % N_CROSS) * GC + cells % GC
    flat_cell = (grid_row * NC + grid_col).astype(jnp.int32)
    grid_source = jnp.zeros((3, NA * NC), jnp.float32).at[:, flat_cell].add(ordered).reshape(3, NA, NC)
    depth_pad = jnp.pad(water_depth, 1)
    water_state = surface
    for substep in range(SUBSTEPS):
        state_pad = jnp.pad(water_state, ((0, 0), (1, 1), (1, 1)))
        water_state = lax_friedrichs(state_pad, depth_pad) + grid_source
    looked = water_state.reshape(3, -1)[:, flat_cell]
    feedback = looked.reshape(3, N_ALONG, N_CROSS, TA, TC, TILE).transpose(0, 1, 3, 2, 4, 5).reshape(3, NTA, NTC, TILE)
    return water_state, density, feedback
```

```python
import math

import jax
import jax.numpy as jnp
from jax import lax
from jax.experimental import pallas as pl
from jax.experimental.pallas import tpu as pltpu
from jax.sharding import PartitionSpec as P

SUBSTEPS = 4
LANES = 128

courant = 0.4
kernel_width = 1.0
LOG2E = math.log2(math.e) / kernel_width

VMEM_LIMIT = 60 * 1024 * 1024


def split(values):
    high = values.astype(jnp.bfloat16).astype(jnp.float32)
    return high, values - high


def vmem():
    return pl.BlockSpec(memory_space=pltpu.MemorySpace.VMEM)


def smem():
    return pl.BlockSpec(memory_space=pltpu.MemorySpace.SMEM)


def columns_of(row):
    return jnp.broadcast_to(row, (LANES, row.shape[1])).T


def sph_kernel(present_ref, pad_ref, density_ref, source_ref, uv_ref, carry_ref, col_ref, acc_ref, sums_ref):
    _, rows2, cols2, size = pad_ref.shape
    rows, cols = rows2 - 2, cols2 - 2
    tiles = rows * cols
    x, y, vx, vy, m = [pad_ref[k] for k in range(5)]
    for d in range(3):
        uv_ref[d] = (2.0 * LOG2E) * (x + (d - 1.0))
        uv_ref[3 + d] = (2.0 * LOG2E) * (y + (d - 1.0))
    gx = [jnp.exp2(-LOG2E * (x + (d - 1.0)) * (x + (d - 1.0))) for d in range(3)]
    gy = [jnp.exp2(-LOG2E * (y + (d - 1.0)) * (y + (d - 1.0))) for d in range(3)]
    for di in range(3):
        for dj in range(3):
            g = gx[di] * gy[dj] * m
            carry_ref[3 * (3 * di + dj)] = g
            carry_ref[3 * (3 * di + dj) + 1] = g * vx
            carry_ref[3 * (3 * di + dj) + 2] = g * vy

    def prepare(t, slot):
        i, j = t // cols, t % cols
        for k in range(2):
            col_ref[slot, k] = columns_of(pad_ref[k, i + 1, pl.ds(j + 1, 1), :])

    def finish(t, slot):
        for k in range(3):
            sums_ref[k, pl.ds(t, 1), :] = jnp.sum(acc_ref[slot, k].T, axis=0, keepdims=True)

    def compute(t, slot):
        i, j = t // cols, t % cols
        half = size // 2
        for h in range(2):
            xa = col_ref[slot, 0, h * half : (h + 1) * half, :]
            ya = col_ref[slot, 1, h * half : (h + 1) * half, :]
            acc = [jnp.zeros((half, size), jnp.float32) for _ in range(3)]
            for w in range(9):
                di, dj = w // 3, w % 3
                there = present_ref[t * 9 + w]
                u = uv_ref[di, i + di, pl.ds(j + dj, 1), :]
                v = uv_ref[3 + dj, i + di, pl.ds(j + dj, 1), :]
                weight = jnp.exp2(xa * u + ya * v)
                for k in range(3):
                    acc[k] = acc[k] + weight * (carry_ref[3 * w + k, i + di, pl.ds(j + dj, 1), :] * there)
            for k in range(3):
                acc_ref[slot, k, h * half : (h + 1) * half, :] = acc[k]

    prepare(0, 0)

    def step(t, _):
        slot = t % 2

        prepare(jnp.minimum(t + 1, tiles - 1), 1 - slot)
        finish(jnp.maximum(t - 1, 0), 1 - slot)
        compute(t, slot)
        return 0

    lax.fori_loop(0, tiles, step, 0)
    finish(tiles - 1, (tiles - 1) % 2)

    for i in range(rows):
        own = pad_ref[:, i + 1, 1 : cols + 1, :]
        outer = jnp.exp2(-LOG2E * (own[0] * own[0] + own[1] * own[1]))
        s0 = outer * sums_ref[0, i * cols : (i + 1) * cols, :]
        s1 = outer * sums_ref[1, i * cols : (i + 1) * cols, :]
        s2 = outer * sums_ref[2, i * cols : (i + 1) * cols, :]
        density = s0 / size
        volume = own[4] / density
        density_ref[i] = density
        source_ref[0, i * cols : (i + 1) * cols, :] = volume
        source_ref[1, i * cols : (i + 1) * cols, :] = volume * (s1 / s0)
        source_ref[2, i * cols : (i + 1) * cols, :] = volume * (s2 / s0)


def sph(padded, present):
    _, rows2, cols2, size = padded.shape
    rows, cols = rows2 - 2, cols2 - 2
    return pl.pallas_call(
        sph_kernel,
        out_shape=(
            jax.ShapeDtypeStruct((rows, cols, size), jnp.float32),
            jax.ShapeDtypeStruct((3, rows * cols, size), jnp.float32),
        ),
        in_specs=[smem(), vmem()],
        out_specs=(vmem(), vmem()),
        scratch_shapes=[
            pltpu.VMEM((6, rows2, cols2, size), jnp.float32),
            pltpu.VMEM((27, rows2, cols2, size), jnp.float32),
            pltpu.VMEM((2, 2, size, size), jnp.float32),
            pltpu.VMEM((2, 3, size, size), jnp.float32),
            pltpu.VMEM((3, rows * cols, size), jnp.float32),
        ],
        compiler_params=pltpu.CompilerParams(vmem_limit_bytes=VMEM_LIMIT),
        name="sph",
    )(present, padded)


def pack_kernel(source_ref, cell_ref, dest_ref, rank_ref, out_ref, left_ref, right_ref, acc_ref, *, group):
    tiles, size = cell_ref.shape
    devices = out_ref.shape[0]
    capacity = right_ref.shape[1]
    acc_ref[...] = jnp.zeros_like(acc_ref)

    def step(b, _):
        for s in range(group):
            t = b * group + s
            at = slice(s * size, (s + 1) * size)
            cell = cell_ref[pl.ds(t, 1), :].astype(jnp.float32)
            upper = jnp.floor(cell * (1.0 / 256.0))
            values = [upper, cell - 256.0 * upper]
            for k in range(3):
                values.extend(split(source_ref[k, pl.ds(t, 1), :]))
            mine = dest_ref[pl.ds(t, 1), :] == lax.broadcasted_iota(jnp.int32, (devices, size), 0)
            for c, value in enumerate(values):
                left_ref[c * devices : (c + 1) * devices, at] = jnp.where(mine, value, 0.0).astype(jnp.bfloat16)
            rank = columns_of(rank_ref[pl.ds(t, 1), :])
            for c in range(capacity // LANES):
                lane = lax.broadcasted_iota(jnp.int32, (size, LANES), 1) + c * LANES
                right_ref[at, c * LANES : (c + 1) * LANES] = jnp.where(rank == lane, 1.0, 0.0).astype(jnp.bfloat16)
        acc_ref[...] += jnp.dot(left_ref[...], right_ref[...], preferred_element_type=jnp.float32)
        return 0

    lax.fori_loop(0, tiles // group, step, 0)

    def part(c):
        return acc_ref[c * devices : (c + 1) * devices, :]

    out_ref[:, 0:capacity] = 256.0 * part(0) + part(1)
    for k in range(3):
        out_ref[:, (k + 1) * capacity : (k + 2) * capacity] = part(2 + 2 * k) + part(3 + 2 * k)


def pack(source, cell, dest, rank, devices, capacity):
    tiles, size = cell.shape
    group = math.gcd(8, tiles)
    return pl.pallas_call(
        lambda *refs: pack_kernel(*refs, group=group),
        out_shape=jax.ShapeDtypeStruct((devices, 4 * capacity), jnp.float32),
        in_specs=[vmem()] * 4,
        out_specs=vmem(),
        scratch_shapes=[
            pltpu.VMEM((8 * devices, group * size), jnp.bfloat16),
            pltpu.VMEM((group * size, capacity), jnp.bfloat16),
            pltpu.VMEM((8 * devices, capacity), jnp.float32),
        ],
        compiler_params=pltpu.CompilerParams(vmem_limit_bytes=VMEM_LIMIT),
        name="pack",
    )(source, cell, dest, rank)


def row_and_col(cell, cells_cross):
    row = jnp.floor((cell + 0.5) * (1.0 / cells_cross))
    return row.astype(jnp.int32), (cell - cells_cross * row).astype(jnp.int32)


def by_load(count, blocks, block, body):
    for n in range(1, blocks + 1):
        low = (n - 1) * block
        fits = (count > low) if n == blocks else (count > low) & (count <= low + block)
        pl.when(fits)(lambda n=n: body(n))


def deposit_kernel(count_ref, in_ref, out_ref, left_ref, right_ref, *, capacity, block):
    _, cells_along, cells_cross = out_ref.shape
    out_ref[...] = jnp.zeros_like(out_ref)

    def sender(s, _):
        def body(n):
            for b in range(n):
                at = slice(b * block, (b + 1) * block)
                row, col = row_and_col(in_ref[pl.ds(s, 1), at], cells_cross)
                mine = row == lax.broadcasted_iota(jnp.int32, (cells_along, block), 0)
                for k in range(3):
                    first = (k + 1) * capacity + b * block
                    for h, value in enumerate(split(in_ref[pl.ds(s, 1), first : first + block])):
                        q = 2 * k + h
                        left_ref[q * cells_along : (q + 1) * cells_along, at] = jnp.where(mine, value, 0.0).astype(
                            jnp.bfloat16
                        )
                for g in range(block // LANES):
                    column = columns_of(col[:, g * LANES : (g + 1) * LANES])
                    for c in range(cells_cross // LANES):
                        lane = lax.broadcasted_iota(jnp.int32, (LANES, LANES), 1) + c * LANES
                        right_ref[b * block + g * LANES : b * block + (g + 1) * LANES, c * LANES : (c + 1) * LANES] = (
                            jnp.where(column == lane, 1.0, 0.0).astype(jnp.bfloat16)
                        )
            for k in range(3):
                both = jnp.dot(
                    left_ref[2 * k * cells_along : (2 * k + 2) * cells_along, 0 : n * block],
                    right_ref[0 : n * block, :],
                    preferred_element_type=jnp.float32,
                )
                out_ref[k] += both[:cells_along] + both[cells_along:]

        by_load(count_ref[s], capacity // block, block, body)
        return 0

    lax.fori_loop(0, in_ref.shape[0], sender, 0)


def deposit(incoming, counts, capacity, cells_along, cells_cross):
    block = math.gcd(256, capacity)
    return pl.pallas_call(
        lambda *refs: deposit_kernel(*refs, capacity=capacity, block=block),
        out_shape=jax.ShapeDtypeStruct((3, cells_along, cells_cross), jnp.float32),
        in_specs=[smem(), vmem()],
        out_specs=vmem(),
        scratch_shapes=[
            pltpu.VMEM((6 * cells_along, capacity), jnp.bfloat16),
            pltpu.VMEM((capacity, cells_cross), jnp.bfloat16),
        ],
        compiler_params=pltpu.CompilerParams(vmem_limit_bytes=VMEM_LIMIT),
        name="deposit",
    )(counts, incoming)


def lookup_kernel(count_ref, in_ref, state_ref, out_ref, left_ref, *, capacity, block):
    _, cells_along, cells_cross = state_ref.shape
    for k in range(3):
        for h, value in enumerate(split(state_ref[k])):
            q = 2 * k + h
            left_ref[q * cells_along : (q + 1) * cells_along, :] = value.astype(jnp.bfloat16)
    out_ref[...] = jnp.zeros_like(out_ref)

    def sender(s, _):
        def body(n):
            for b in range(n):
                row, col = row_and_col(in_ref[pl.ds(s, 1), b * block : (b + 1) * block], cells_cross)
                mine = row == lax.broadcasted_iota(jnp.int32, (cells_along, block), 0)
                right = jnp.where(
                    col == lax.broadcasted_iota(jnp.int32, (cells_cross, block), 0), 1.0, 0.0
                ).astype(jnp.bfloat16)
                for k in range(3):
                    both = jnp.dot(
                        left_ref[2 * k * cells_along : (2 * k + 2) * cells_along, :],
                        right,
                        preferred_element_type=jnp.float32,
                    )
                    chosen = jnp.where(mine, both[:cells_along] + both[cells_along:], 0.0)
                    first = k * capacity + b * block
                    out_ref[pl.ds(s, 1), first : first + block] = jnp.sum(chosen, axis=0, keepdims=True)

        by_load(count_ref[s], capacity // block, block, body)
        return 0

    lax.fori_loop(0, in_ref.shape[0], sender, 0)


def lookup(incoming, counts, state, capacity):
    devices = incoming.shape[0]
    _, cells_along, cells_cross = state.shape
    block = math.gcd(256, capacity)
    return pl.pallas_call(
        lambda *refs: lookup_kernel(*refs, capacity=capacity, block=block),
        out_shape=jax.ShapeDtypeStruct((devices, 3 * capacity), jnp.float32),
        in_specs=[smem(), vmem(), vmem()],
        out_specs=vmem(),
        scratch_shapes=[pltpu.VMEM((6 * cells_along, cells_cross), jnp.bfloat16)],
        compiler_params=pltpu.CompilerParams(vmem_limit_bytes=VMEM_LIMIT),
        name="lookup",
    )(counts, incoming, state)


def unpack_kernel(in_ref, dest_ref, rank_ref, out_ref, left_ref, *, capacity, group):
    tiles, size = dest_ref.shape
    devices = in_ref.shape[0]
    for k in range(3):
        for h, value in enumerate(split(in_ref[:, k * capacity : (k + 1) * capacity])):
            q = 2 * k + h
            left_ref[q * devices : (q + 1) * devices, :] = value.astype(jnp.bfloat16)

    def step(b, _):
        for s in range(group):
            t = b * group + s
            right = jnp.where(
                rank_ref[pl.ds(t, 1), :] == lax.broadcasted_iota(jnp.int32, (capacity, size), 0), 1.0, 0.0
            ).astype(jnp.bfloat16)
            mine = dest_ref[pl.ds(t, 1), :] == lax.broadcasted_iota(jnp.int32, (devices, size), 0)
            every = jnp.dot(left_ref[...], right, preferred_element_type=jnp.float32)
            for k in range(3):
                both = every[2 * k * devices : (2 * k + 1) * devices] + every[(2 * k + 1) * devices : (2 * k + 2) * devices]
                out_ref[k, pl.ds(t, 1), :] = jnp.sum(jnp.where(mine, both, 0.0), axis=0, keepdims=True)
        return 0

    lax.fori_loop(0, tiles // group, step, 0)


def unpack(returned, dest, rank, capacity):
    tiles, size = dest.shape
    devices = returned.shape[0]
    group = math.gcd(4, tiles)
    return pl.pallas_call(
        lambda *refs: unpack_kernel(*refs, capacity=capacity, group=group),
        out_shape=jax.ShapeDtypeStruct((3, tiles, size), jnp.float32),
        in_specs=[vmem()] * 3,
        out_specs=vmem(),
        scratch_shapes=[pltpu.VMEM((6 * devices, capacity), jnp.bfloat16)],
        compiler_params=pltpu.CompilerParams(vmem_limit_bytes=VMEM_LIMIT),
        name="unpack",
    )(returned, dest, rank)


def swap(axis, to_next, to_previous):
    count = lax.axis_size(axis)
    before = lax.ppermute(to_next, axis, [(i, i + 1) for i in range(count - 1)])
    after = lax.ppermute(to_previous, axis, [(i + 1, i) for i in range(count - 1)])
    return before, after


def padded_together(fields):
    arrays = [array for array, _, _ in fields]
    for step, axis in enumerate(("along", "cross")):
        heads, tails = [], []
        for array, (_, dims, width) in zip(arrays, fields):
            dim = dims[step]
            heads.append(lax.slice_in_dim(array, 0, width, axis=dim))
            tails.append(lax.slice_in_dim(array, array.shape[dim] - width, array.shape[dim], axis=dim))
        flat = lambda parts: jnp.concatenate([part.reshape(-1) for part in parts])
        before, after = swap(axis, flat(tails), flat(heads))
        start, grown = 0, []
        for array, head, (_, dims, _) in zip(arrays, heads, fields):
            rims = [rim[start : start + head.size].reshape(head.shape) for rim in (before, after)]
            start += head.size
            grown.append(jnp.concatenate([rims[0], array, rims[1]], axis=dims[step]))
        arrays = grown
    return arrays


def lax_friedrichs(state_pad, depth_pad):
    height = state_pad[0]
    speed_x = state_pad[1]
    speed_y = state_pad[2]
    flux_x = depth_pad * speed_x
    flux_y = depth_pad * speed_y

    def average(quantity):
        return 0.25 * (quantity[2:, 1:-1] + quantity[:-2, 1:-1] + quantity[1:-1, 2:] + quantity[1:-1, :-2])

    next_height = average(height) - 0.5 * courant * (
        flux_x[2:, 1:-1] - flux_x[:-2, 1:-1] + flux_y[1:-1, 2:] - flux_y[1:-1, :-2]
    )
    next_speed_x = average(speed_x) - 0.5 * courant * (height[2:, 1:-1] - height[:-2, 1:-1])
    next_speed_y = average(speed_y) - 0.5 * courant * (height[1:-1, 2:] - height[1:-1, :-2])
    return jnp.stack([next_height, next_speed_x, next_speed_y])


def slot_ranks(destination, devices):
    groups, block = destination.shape
    onehot = (destination[:, :, None] == jnp.arange(devices, dtype=jnp.int32)).astype(jnp.bfloat16)
    lower = (jnp.arange(block)[:, None] > jnp.arange(block)[None, :]).astype(jnp.bfloat16)
    earlier = jnp.einsum("ij,bjd->bid", lower, onehot, preferred_element_type=jnp.float32)
    counts = jnp.sum(onehot.astype(jnp.float32), axis=1)
    before = jnp.cumsum(counts, axis=0) - counts
    return jnp.sum(onehot.astype(jnp.float32) * (earlier + before[:, None, :]), axis=2).astype(jnp.int32)


def shards(offsets, velocity, particle_mass, neighbours, owner_device, target_cell, surface, water_depth):
    _, tiles_along, tiles_cross, tile_size = offsets.shape
    _, cells_along, cells_cross = surface.shape
    along_count = lax.axis_size("along")
    cross_count = lax.axis_size("cross")
    devices = along_count * cross_count
    tiles = tiles_along * tiles_cross
    particles = tiles * tile_size
    capacity = -(-3 * particles // devices // LANES) * LANES
    margin = SUBSTEPS

    stacked = jnp.concatenate([offsets, velocity, particle_mass[None]], axis=0)
    water = jnp.concatenate([surface, water_depth[None]], axis=0)
    padded, wide_water = padded_together([(stacked, (1, 2), 1), (water, (1, 2), margin)])

    destination = owner_device.reshape(tiles, tile_size)
    cell = target_cell.reshape(tiles, tile_size)
    rank = slot_ranks(destination, devices)
    present = jnp.any(neighbours[..., :, None] == jnp.arange(9, dtype=jnp.int32), axis=-2).astype(jnp.float32)

    density, sources = sph(padded, present.reshape(-1))
    outgoing = pack(sources, cell, destination, rank, devices, capacity)
    incoming = lax.all_to_all(outgoing, ("along", "cross"), split_axis=0, concat_axis=0, tiled=True)
    counts = jnp.sum((incoming[:, capacity : 2 * capacity] != 0.0).astype(jnp.int32), axis=1)
    grid_source = deposit(incoming, counts, capacity, cells_along, cells_cross)
    (wide_source,) = padded_together([(grid_source, (1, 2), margin)])

    rows_global = (
        lax.axis_index("along") * cells_along - margin + jnp.arange(cells_along + 2 * margin, dtype=jnp.int32)
    )
    cols_global = (
        lax.axis_index("cross") * cells_cross - margin + jnp.arange(cells_cross + 2 * margin, dtype=jnp.int32)
    )
    inside_rows = (rows_global >= 0) & (rows_global < cells_along * along_count)
    inside_cols = (cols_global >= 0) & (cols_global < cells_cross * cross_count)
    inside = (inside_rows[:, None] & inside_cols[None, :]).astype(jnp.float32)
    wide_state = wide_water[:3]
    depth_pad = jnp.pad(wide_water[3], 1)
    for _ in range(SUBSTEPS):
        state_pad = jnp.pad(wide_state, ((0, 0), (1, 1), (1, 1)))
        wide_state = (lax_friedrichs(state_pad, depth_pad) + wide_source) * inside
    water_state = wide_state[:, margin : margin + cells_along, margin : margin + cells_cross]

    looked = lookup(incoming, counts, water_state, capacity)
    returned = lax.all_to_all(looked, ("along", "cross"), split_axis=0, concat_axis=0, tiled=True)
    feedback = unpack(returned, destination, rank, capacity)
    return water_state, density, feedback.reshape(3, tiles_along, tiles_cross, tile_size)


def solution(mesh):
    in_specs = (
        P(None, "along", "cross", None),
        P(None, "along", "cross", None),
        P("along", "cross", None),
        P("along", "cross", None),
        P("along", "cross", None, None),
        P("along", "cross", None),
        P(None, "along", "cross"),
        P("along", "cross"),
    )
    out_specs = (
        P(None, "along", "cross"),
        P("along", "cross", None),
        P(None, "along", "cross", None),
    )
    return jax.shard_map(shards, mesh=mesh, in_specs=in_specs, out_specs=out_specs, check_vma=False)
```

```python
import math

import jax
import jax.numpy as jnp
from jax import lax
from jax.experimental import pallas as pl
from jax.experimental.pallas import tpu as pltpu
from jax.sharding import PartitionSpec as P

SUBSTEPS = 4
LANES = 128

courant = 0.4
kernel_width = 1.0
LOG2E = math.log2(math.e) / kernel_width

VMEM_LIMIT = 60 * 1024 * 1024


def split(values):
    high = values.astype(jnp.bfloat16).astype(jnp.float32)
    return high, values - high


def vmem():
    return pl.BlockSpec(memory_space=pltpu.MemorySpace.VMEM)


def smem():
    return pl.BlockSpec(memory_space=pltpu.MemorySpace.SMEM)


def one_hot(index, count):
    size = math.gcd(LANES, count)
    rows = lax.broadcasted_iota(jnp.int32, (size, index.shape[1]), 0).astype(jnp.float32).astype(jnp.bfloat16)
    parts = []
    for first in range(0, count, size):
        here = index - first
        here = jnp.where((here >= 0.0) & (here < size), here, -1.0).astype(jnp.bfloat16)
        parts.append(jnp.where(here == rows, jnp.bfloat16(1), jnp.bfloat16(0)))
    return parts[0] if len(parts) == 1 else jnp.concatenate(parts, axis=0)


def one_hot_t(index, count):
    upper = jnp.floor(index * (1.0 / LANES))
    code = LANES + index - LANES * upper
    for n in range(1, count // LANES):
        code = jnp.where(upper >= n, 2.0 * code, code)
    code = jnp.broadcast_to(code.astype(jnp.bfloat16), (LANES, LANES)).T
    lane = (LANES + lax.broadcasted_iota(jnp.int32, (LANES, LANES), 1)).astype(jnp.float32)
    return jnp.concatenate(
        [
            jnp.where(code == (lane * 2.0**n).astype(jnp.bfloat16), jnp.bfloat16(1), jnp.bfloat16(0))
            for n in range(count // LANES)
        ],
        axis=1,
    )


def is_row(index, count):
    rows = lax.broadcasted_iota(jnp.int32, (count, index.shape[1]), 0).astype(jnp.float32).astype(jnp.bfloat16)
    return jnp.where((index >= 0.0) & (index < count), index, -1.0).astype(jnp.bfloat16) == rows


def columns_of(row):
    return jnp.broadcast_to(row, (LANES, row.shape[1])).T


def sph_kernel(present_ref, pad_ref, density_ref, source_ref, uv_ref, carry_ref, col_ref, acc_ref, sums_ref):
    _, rows2, cols2, size = pad_ref.shape
    rows, cols = rows2 - 2, cols2 - 2
    tiles = rows * cols
    x, y, vx, vy, m = [pad_ref[k] for k in range(5)]
    for d in range(3):
        uv_ref[d] = (2.0 * LOG2E) * (x + (d - 1.0))
        uv_ref[3 + d] = (2.0 * LOG2E) * (y + (d - 1.0))
    gx = [jnp.exp2(-LOG2E * (x + (d - 1.0)) * (x + (d - 1.0))) for d in range(3)]
    gy = [jnp.exp2(-LOG2E * (y + (d - 1.0)) * (y + (d - 1.0))) for d in range(3)]
    for di in range(3):
        for dj in range(3):
            g = gx[di] * gy[dj] * m
            carry_ref[3 * (3 * di + dj)] = g
            carry_ref[3 * (3 * di + dj) + 1] = g * vx
            carry_ref[3 * (3 * di + dj) + 2] = g * vy

    def prepare(t, slot):
        i, j = t // cols, t % cols
        for k in range(2):
            col_ref[slot, k] = columns_of(pad_ref[k, i + 1, pl.ds(j + 1, 1), :])

    def finish(t, slot):
        for k in range(3):
            sums_ref[k, pl.ds(t, 1), :] = jnp.sum(acc_ref[slot, k].T, axis=0, keepdims=True)

    def compute(t, slot):
        i, j = t // cols, t % cols
        half = size // 2
        for h in range(2):
            xa = col_ref[slot, 0, h * half : (h + 1) * half, :]
            ya = col_ref[slot, 1, h * half : (h + 1) * half, :]
            acc = [jnp.zeros((half, size), jnp.float32) for _ in range(3)]
            for w in range(9):
                di, dj = w // 3, w % 3
                there = present_ref[t * 9 + w]
                u = uv_ref[di, i + di, pl.ds(j + dj, 1), :]
                v = uv_ref[3 + dj, i + di, pl.ds(j + dj, 1), :]
                weight = jnp.exp2(xa * u + ya * v)
                for k in range(3):
                    acc[k] = acc[k] + weight * (carry_ref[3 * w + k, i + di, pl.ds(j + dj, 1), :] * there)
            for k in range(3):
                acc_ref[slot, k, h * half : (h + 1) * half, :] = acc[k]

    prepare(0, 0)

    def step(p, _):
        for slot in range(2):
            t = 2 * p + slot
            prepare(jnp.minimum(t + 1, tiles - 1), 1 - slot)
            finish(jnp.maximum(t - 1, 0), 1 - slot)
            compute(t, slot)
        return 0

    lax.fori_loop(0, tiles // 2, step, 0)
    finish(tiles - 1, (tiles - 1) % 2)

    for i in range(rows):
        own = pad_ref[:, i + 1, 1 : cols + 1, :]
        outer = jnp.exp2(-LOG2E * (own[0] * own[0] + own[1] * own[1]))
        s0 = outer * sums_ref[0, i * cols : (i + 1) * cols, :]
        s1 = outer * sums_ref[1, i * cols : (i + 1) * cols, :]
        s2 = outer * sums_ref[2, i * cols : (i + 1) * cols, :]
        density = s0 / size
        volume = own[4] / density
        density_ref[i] = density
        source_ref[0, i * cols : (i + 1) * cols, :] = volume
        source_ref[1, i * cols : (i + 1) * cols, :] = volume * (s1 / s0)
        source_ref[2, i * cols : (i + 1) * cols, :] = volume * (s2 / s0)


def sph(padded, present):
    _, rows2, cols2, size = padded.shape
    rows, cols = rows2 - 2, cols2 - 2
    return pl.pallas_call(
        sph_kernel,
        out_shape=(
            jax.ShapeDtypeStruct((rows, cols, size), jnp.float32),
            jax.ShapeDtypeStruct((3, rows * cols, size), jnp.float32),
        ),
        in_specs=[smem(), vmem()],
        out_specs=(vmem(), vmem()),
        scratch_shapes=[
            pltpu.VMEM((6, rows2, cols2, size), jnp.float32),
            pltpu.VMEM((27, rows2, cols2, size), jnp.float32),
            pltpu.VMEM((2, 2, size, size), jnp.float32),
            pltpu.VMEM((2, 3, size, size), jnp.float32),
            pltpu.VMEM((3, rows * cols, size), jnp.float32),
        ],
        compiler_params=pltpu.CompilerParams(vmem_limit_bytes=VMEM_LIMIT),
        name="sph",
    )(present, padded)


def pack_kernel(source_ref, cell_ref, dest_ref, rank_ref, out_ref, acc_ref, *, group):
    tiles, size = cell_ref.shape
    devices = out_ref.shape[0]
    capacity = acc_ref.shape[1]
    acc_ref[...] = jnp.zeros_like(acc_ref)

    def work(b, _):
        lefts, rights = [], []
        for s in range(group):
            t = b * group + s
            cell = cell_ref[pl.ds(t, 1), :].astype(jnp.float32)
            upper = jnp.floor(cell * (1.0 / 256.0))
            values = [upper, cell - 256.0 * upper]
            for k in range(3):
                values.extend(split(source_ref[k, pl.ds(t, 1), :]))
            mine = is_row(dest_ref[pl.ds(t, 1), :].astype(jnp.float32), devices)
            lefts.append(
                jnp.concatenate(
                    [jnp.where(mine, value.astype(jnp.bfloat16), jnp.bfloat16(0)) for value in values], axis=0
                )
            )
            rights.append(one_hot(rank_ref[pl.ds(t, 1), :].astype(jnp.float32), capacity))
        acc_ref[...] += lax.dot_general(
            jnp.concatenate(lefts, axis=1),
            jnp.concatenate(rights, axis=1),
            (((1,), (1,)), ((), ())),
            preferred_element_type=jnp.float32,
        )
        return 0

    lax.fori_loop(0, tiles // group, work, 0)

    def part(c):
        return acc_ref[c * devices : (c + 1) * devices, :]

    outs = [256.0 * part(0) + part(1)] + [part(2 + 2 * k) + part(3 + 2 * k) for k in range(3)]
    blocks = capacity // LANES
    for k, out in enumerate(outs):
        for b in range(blocks):
            out_ref[:, k * blocks + b, :] = out[:, b * LANES : (b + 1) * LANES]


def pack(source, cell, dest, rank, devices, capacity):
    tiles, size = cell.shape
    group = math.gcd(16, tiles)
    return pl.pallas_call(
        lambda *refs: pack_kernel(*refs, group=group),
        out_shape=jax.ShapeDtypeStruct((devices, 4 * capacity // LANES, LANES), jnp.float32),
        in_specs=[vmem()] * 4,
        out_specs=vmem(),
        scratch_shapes=[pltpu.VMEM((8 * devices, capacity), jnp.float32)],
        compiler_params=pltpu.CompilerParams(vmem_limit_bytes=VMEM_LIMIT),
        name="pack",
    )(source, cell, dest, rank)


def row_and_col(cell, cells_cross):
    row = jnp.floor((cell + 0.5) * (1.0 / cells_cross))
    return row, cell - cells_cross * row


GROUP = 16


def list_blocks(start_ref, amount_ref, block_ref, bound_ref, *, senders, bins, blocks):
    total = 0
    together = math.gcd(8, senders)
    for q in range(bins):

        def some(g, total):
            for n in range(together):
                s = g * together + n
                first = 4 * blocks * s + start_ref[s * bins + q]
                for b in range(blocks):
                    block_ref[total + b] = first + b
                total = total + amount_ref[s * bins + q]
            return total

        total = lax.fori_loop(0, senders // together, some, total)
        for b in range(GROUP):
            block_ref[total + b] = -1
        total = (total + GROUP - 1) // GROUP * GROUP
        bound_ref[q] = total // GROUP
    for b in range(3 * GROUP):
        block_ref[total + b] = -1


def list_sizes(senders, bins, blocks):
    return senders * (blocks + bins) + (bins + 4) * GROUP, bins


def bin_of(group, bound_ref, bins):
    q = 0
    for n in range(bins - 1):
        q = q + (group >= bound_ref[n]).astype(jnp.int32)
    return q


def by_group(bound_ref, bins, work):
    def pair(p, _):
        for n in range(2):
            work(2 * p + n)
        return 0

    lax.fori_loop(0, (bound_ref[bins - 1] + 1) // 2, pair, 0)


def block_cells(in_ref, row, base, cells_cross):
    there = jnp.maximum(row, 0)
    row_of, col_of = row_and_col(in_ref[pl.ds(there, 1), :], cells_cross)
    return there, row_of - jnp.where(row < 0, 1 << 20, base).astype(jnp.float32), col_of


def deposit_kernel(start_ref, amount_ref, in_ref, out_ref, block_ref, bound_ref, *, senders, bins, blocks):
    _, cells_along, cells_cross = out_ref.shape
    height = cells_along // bins
    list_blocks(start_ref, amount_ref, block_ref, bound_ref, senders=senders, bins=bins, blocks=blocks)
    out_ref[...] = jnp.zeros_like(out_ref)

    def work(group):
        base = bin_of(group, bound_ref, bins) * height
        lefts, rights = [], []
        for b in range(GROUP):
            row, row_of, col_of = block_cells(in_ref, block_ref[group * GROUP + b], base, cells_cross)
            mine = is_row(row_of, height)
            values = [part for k in range(3) for part in split(in_ref[pl.ds(row + (k + 1) * blocks, 1), :])]
            lefts.append(
                jnp.concatenate(
                    [jnp.where(mine, value.astype(jnp.bfloat16), jnp.bfloat16(0)) for value in values], axis=0
                )
            )
            rights.append(one_hot_t(col_of, cells_cross))
        both = jnp.dot(
            jnp.concatenate(lefts, axis=1), jnp.concatenate(rights, axis=0), preferred_element_type=jnp.float32
        )
        for k in range(3):
            part = both[2 * k * height : (2 * k + 1) * height] + both[(2 * k + 1) * height : (2 * k + 2) * height]
            out_ref[k, pl.ds(pl.multiple_of(base, height), height), :] += part

    by_group(bound_ref, bins, work)


def deposit(incoming, starts, amounts, bins, cells_along, cells_cross):
    senders = incoming.shape[0]
    blocks = incoming.shape[1] // 4
    size, bounds = list_sizes(senders, bins, blocks)
    return pl.pallas_call(
        lambda *refs: deposit_kernel(*refs, senders=senders, bins=bins, blocks=blocks),
        out_shape=(
            jax.ShapeDtypeStruct((3, cells_along, cells_cross), jnp.float32),
            jax.ShapeDtypeStruct((size,), jnp.int32),
            jax.ShapeDtypeStruct((bounds,), jnp.int32),
        ),
        in_specs=[smem(), smem(), vmem()],
        out_specs=(vmem(), smem(), smem()),
        compiler_params=pltpu.CompilerParams(vmem_limit_bytes=VMEM_LIMIT),
        name="deposit",
    )(starts, amounts, incoming.reshape(-1, LANES))


def substeps(edge_ref, water_ref, source_ref, state_ref, margin):
    _, cells_along, cells_cross = state_ref.shape
    _, height, width = water_ref.shape
    rows = lax.broadcasted_iota(jnp.int32, (height, width), 0)
    cols = lax.broadcasted_iota(jnp.int32, (height, width), 1)
    inside = (rows >= edge_ref[0]) & (rows < edge_ref[1]) & (cols >= edge_ref[2]) & (cols < edge_ref[3])

    def along(field):
        return pltpu.roll(field, height - 1, 0), pltpu.roll(field, 1, 0)

    def cross(field):
        return pltpu.roll(field, width - 1, 1), pltpu.roll(field, 1, 1)

    depth = water_ref[3]
    elevation, speed_x, speed_y = water_ref[0], water_ref[1], water_ref[2]
    for _ in range(SUBSTEPS):
        east, west = along(elevation)
        north, south = cross(elevation)
        flux_east, flux_west = along(depth * speed_x)
        flux_north, flux_south = cross(depth * speed_y)
        around = [sum(along(f) + cross(f)) for f in (speed_x, speed_y)]
        flow = flux_east - flux_west + flux_north - flux_south
        following = (
            0.25 * (east + west + north + south) - 0.5 * courant * flow,
            0.25 * around[0] - 0.5 * courant * (east - west),
            0.25 * around[1] - 0.5 * courant * (north - south),
        )
        elevation, speed_x, speed_y = [
            jnp.where(inside, value + source_ref[k], 0.0) for k, value in enumerate(following)
        ]
    for k, field in enumerate((elevation, speed_x, speed_y)):
        field = pltpu.roll(pltpu.roll(field, height - margin, 0), width - margin, 1)
        state_ref[k] = field[:cells_along, :cells_cross]


def lookup_kernel(
    block_ref, bound_ref, edge_ref, in_ref, water_ref, source_ref, out_ref, state_ref, left_ref, *, bins, blocks, margin
):
    _, cells_along, cells_cross = state_ref.shape
    height = cells_along // bins
    substeps(edge_ref, water_ref, source_ref, state_ref, margin)
    for k in range(3):
        for h, value in enumerate(split(state_ref[k])):
            q = 2 * k + h
            for n in range(bins):
                left_ref[n, q * height : (q + 1) * height, :] = value[n * height : (n + 1) * height].astype(jnp.bfloat16)
    out_ref[...] = jnp.zeros_like(out_ref)

    def work(group):
        q = bin_of(group, bound_ref, bins)
        right = jnp.concatenate(
            [
                one_hot(block_cells(in_ref, block_ref[group * GROUP + b], 0, cells_cross)[2], cells_cross)
                for b in range(GROUP)
            ],
            axis=1,
        )
        every = jnp.dot(left_ref[q], right, preferred_element_type=jnp.float32)
        for b in range(GROUP):
            at = slice(b * LANES, (b + 1) * LANES)
            row, row_of, _ = block_cells(in_ref, block_ref[group * GROUP + b], q * height, cells_cross)
            mine = row_of == lax.broadcasted_iota(jnp.int32, (height, LANES), 0).astype(jnp.float32)
            for k in range(3):
                both = every[2 * k * height : (2 * k + 1) * height, at] + every[(2 * k + 1) * height : (2 * k + 2) * height, at]
                found = jnp.sum(jnp.where(mine, both, 0.0), axis=0, keepdims=True)
                out_ref[pl.ds(row - row // (4 * blocks) * blocks + k * blocks, 1), :] += found

    by_group(bound_ref, bins, work)


def lookup(incoming, block_list, bounds, edges, water, source, bins, margin, cells_along, cells_cross):
    senders, rows, _ = incoming.shape
    return pl.pallas_call(
        lambda *refs: lookup_kernel(*refs, bins=bins, blocks=rows // 4, margin=margin),
        out_shape=(
            jax.ShapeDtypeStruct((senders * rows // 4 * 3, LANES), jnp.float32),
            jax.ShapeDtypeStruct((3, cells_along, cells_cross), jnp.float32),
        ),
        in_specs=[smem()] * 3 + [vmem()] * 3,
        out_specs=(vmem(), vmem()),
        scratch_shapes=[pltpu.VMEM((bins, 6 * cells_along // bins, cells_cross), jnp.bfloat16)],
        compiler_params=pltpu.CompilerParams(vmem_limit_bytes=VMEM_LIMIT),
        name="lookup",
    )(block_list, bounds, edges, incoming.reshape(-1, LANES), water, source)


def unpack_kernel(in_ref, dest_ref, rank_ref, out_ref, left_ref, *, capacity, group):
    tiles, size = dest_ref.shape
    blocks = capacity // LANES
    devices = in_ref.shape[0] // (3 * blocks)
    for k in range(3):
        for b in range(blocks):
            for h, value in enumerate(split(in_ref[pl.ds(k * blocks + b, devices, stride=3 * blocks), :])):
                q = 2 * k + h
                left_ref[q * devices : (q + 1) * devices, b * LANES : (b + 1) * LANES] = value.astype(jnp.bfloat16)

    def step(b, _):
        right = jnp.concatenate(
            [one_hot(rank_ref[pl.ds(b * group + s, 1), :].astype(jnp.float32), capacity) for s in range(group)], axis=1
        )
        every = jnp.dot(left_ref[...], right, preferred_element_type=jnp.float32)
        for s in range(group):
            t = b * group + s
            at = slice(s * size, (s + 1) * size)
            mine = dest_ref[pl.ds(t, 1), :] == lax.broadcasted_iota(jnp.int32, (devices, size), 0)
            for k in range(3):
                both = every[2 * k * devices : (2 * k + 1) * devices, at]
                both = both + every[(2 * k + 1) * devices : (2 * k + 2) * devices, at]
                out_ref[k, pl.ds(t, 1), :] = jnp.sum(jnp.where(mine, both, 0.0), axis=0, keepdims=True)
        return 0

    lax.fori_loop(0, tiles // group, step, 0)


def unpack(returned, dest, rank, capacity):
    tiles, size = dest.shape
    devices = returned.shape[0] * LANES // (3 * capacity)
    group = math.gcd(16, tiles)
    return pl.pallas_call(
        lambda *refs: unpack_kernel(*refs, capacity=capacity, group=group),
        out_shape=jax.ShapeDtypeStruct((3, tiles, size), jnp.float32),
        in_specs=[vmem()] * 3,
        out_specs=vmem(),
        scratch_shapes=[pltpu.VMEM((6 * devices, capacity), jnp.bfloat16)],
        compiler_params=pltpu.CompilerParams(vmem_limit_bytes=VMEM_LIMIT),
        name="unpack",
    )(returned, dest, rank)


def swap(axis, to_next, to_previous):
    count = lax.axis_size(axis)
    before = lax.ppermute(to_next, axis, [(i, i + 1) for i in range(count - 1)])
    after = lax.ppermute(to_previous, axis, [(i + 1, i) for i in range(count - 1)])
    return before, after


def padded_together(fields):
    arrays = [array for array, _, _ in fields]
    for step, axis in enumerate(("along", "cross")):
        heads, tails = [], []
        for array, (_, dims, width) in zip(arrays, fields):
            dim = dims[step]
            heads.append(lax.slice_in_dim(array, 0, width, axis=dim))
            tails.append(lax.slice_in_dim(array, array.shape[dim] - width, array.shape[dim], axis=dim))
        flat = lambda parts: jnp.concatenate([part.reshape(-1) for part in parts])
        before, after = swap(axis, flat(tails), flat(heads))
        start, grown = 0, []
        for array, head, (_, dims, _) in zip(arrays, heads, fields):
            rims = [rim[start : start + head.size].reshape(head.shape) for rim in (before, after)]
            start += head.size
            grown.append(jnp.concatenate([rims[0], array, rims[1]], axis=dims[step]))
        arrays = grown
    return arrays


def slot_ranks(key, destination, devices, bins):
    groups, block = key.shape
    onehot = (key[:, :, None] == jnp.arange(devices * bins, dtype=jnp.int32)).astype(jnp.bfloat16)
    lower = (jnp.arange(block)[:, None] > jnp.arange(block)[None, :]).astype(jnp.bfloat16)
    earlier = jnp.einsum("ij,bjd->bid", lower, onehot, preferred_element_type=jnp.float32)
    counts = jnp.sum(onehot.astype(jnp.float32), axis=1)
    totals = jnp.sum(counts, axis=0).reshape(devices, bins)
    first = (jnp.cumsum(totals, axis=1) - totals).reshape(-1)
    before = jnp.cumsum(counts, axis=0) - counts + first
    return jnp.sum(onehot.astype(jnp.float32) * (earlier + before[:, None, :]), axis=2).astype(jnp.int32)


def shards(offsets, velocity, particle_mass, neighbours, owner_device, target_cell, surface, water_depth):
    _, tiles_along, tiles_cross, tile_size = offsets.shape
    _, cells_along, cells_cross = surface.shape
    along_count = lax.axis_size("along")
    cross_count = lax.axis_size("cross")
    devices = along_count * cross_count
    tiles = tiles_along * tiles_cross
    particles = tiles * tile_size
    capacity = -(-3 * particles // devices // LANES) * LANES
    margin = SUBSTEPS

    stacked = jnp.concatenate([offsets, velocity, particle_mass[None]], axis=0)
    water = jnp.concatenate([surface, water_depth[None]], axis=0)
    padded, wide_water = padded_together([(stacked, (1, 2), 1), (water, (1, 2), margin)])

    destination = owner_device.reshape(tiles, tile_size)
    cell = target_cell.reshape(tiles, tile_size)
    bins = max(1, min(4, LANES // devices))
    rank = slot_ranks(destination * bins + cell // (cells_along * cells_cross // bins), destination, devices, bins)
    present = jnp.any(neighbours[..., :, None] == jnp.arange(9, dtype=jnp.int32), axis=-2).astype(jnp.float32)

    density, sources = sph(padded, present.reshape(-1))
    outgoing = pack(sources, cell, destination, rank, devices, capacity)
    incoming = lax.all_to_all(outgoing, ("along", "cross"), split_axis=0, concat_axis=0, tiled=True)
    blocks = capacity // LANES
    filled = incoming[:, blocks : 2 * blocks] != 0.0
    bin_in = jnp.floor(incoming[:, :blocks] * (bins / (cells_along * cells_cross)))
    counts = jnp.stack([jnp.sum((filled & (bin_in == q)).astype(jnp.int32), axis=(1, 2)) for q in range(bins)], axis=1)
    ends = jnp.cumsum(counts, axis=1)
    starts = (ends - counts) // LANES
    amounts = jnp.where(counts > 0, (ends + LANES - 1) // LANES - starts, 0)
    grid_source, block_list, bounds = deposit(
        incoming, starts.reshape(-1), amounts.reshape(-1), bins, cells_along, cells_cross
    )
    (wide_source,) = padded_together([(grid_source, (1, 2), margin)])

    edges = []
    for axis, length in (("along", cells_along), ("cross", cells_cross)):
        place = lax.axis_index(axis)
        edges.append(jnp.where(place == 0, margin, 0))
        edges.append(jnp.where(place == lax.axis_size(axis) - 1, length + margin, length + 2 * margin))
    to_lanes = [(0, 0), (0, 0), (0, -(cells_cross + 2 * margin) % LANES)]
    looked, water_state = lookup(
        incoming,
        block_list,
        bounds,
        jnp.stack(edges).astype(jnp.int32),
        jnp.pad(wide_water, to_lanes),
        jnp.pad(wide_source, to_lanes),
        bins,
        margin,
        cells_along,
        cells_cross,
    )
    returned = lax.all_to_all(
        looked.reshape(devices, 3 * capacity), ("along", "cross"), split_axis=0, concat_axis=0, tiled=True
    ).reshape(looked.shape)
    feedback = unpack(returned, destination, rank, capacity)
    return water_state, density, feedback.reshape(3, tiles_along, tiles_cross, tile_size)


def solution(mesh):
    in_specs = (
        P(None, "along", "cross", None),
        P(None, "along", "cross", None),
        P("along", "cross", None),
        P("along", "cross", None),
        P("along", "cross", None, None),
        P("along", "cross", None),
        P(None, "along", "cross"),
        P("along", "cross"),
    )
    out_specs = (
        P(None, "along", "cross"),
        P("along", "cross", None),
        P(None, "along", "cross", None),
    )
    return jax.shard_map(shards, mesh=mesh, in_specs=in_specs, out_specs=out_specs, check_vma=False)
```

```python
import math

import jax
import jax.numpy as jnp
from jax import lax
from jax.experimental import pallas as pl
from jax.experimental.pallas import tpu as pltpu
from jax.sharding import PartitionSpec as P

SUBSTEPS = 4
LANES = 128

courant = 0.4
kernel_width = 1.0
LOG2E = math.log2(math.e) / kernel_width

VMEM_LIMIT = 60 * 1024 * 1024


def split(values):
    high = values.astype(jnp.bfloat16).astype(jnp.float32)
    return high, values - high


def vmem():
    return pl.BlockSpec(memory_space=pltpu.MemorySpace.VMEM)


def smem():
    return pl.BlockSpec(memory_space=pltpu.MemorySpace.SMEM)


def one_hot(index, count):
    size = math.gcd(LANES, count)
    rows = lax.broadcasted_iota(jnp.int32, (size, index.shape[1]), 0).astype(jnp.float32).astype(jnp.bfloat16)
    parts = []
    for first in range(0, count, size):
        here = index - first
        here = jnp.where((here >= 0.0) & (here < size), here, -1.0).astype(jnp.bfloat16)
        parts.append(jnp.where(here == rows, jnp.bfloat16(1), jnp.bfloat16(0)))
    return parts[0] if len(parts) == 1 else jnp.concatenate(parts, axis=0)


def one_hot_t(index, count):
    upper = jnp.floor(index * (1.0 / LANES))
    code = LANES + index - LANES * upper
    for n in range(1, count // LANES):
        code = jnp.where(upper >= n, 2.0 * code, code)
    code = jnp.broadcast_to(code.astype(jnp.bfloat16), (LANES, LANES)).T
    lane = (LANES + lax.broadcasted_iota(jnp.int32, (LANES, LANES), 1)).astype(jnp.float32)
    return jnp.concatenate(
        [
            jnp.where(code == (lane * 2.0**n).astype(jnp.bfloat16), jnp.bfloat16(1), jnp.bfloat16(0))
            for n in range(count // LANES)
        ],
        axis=1,
    )


def is_row(index, count):
    rows = lax.broadcasted_iota(jnp.int32, (count, index.shape[1]), 0).astype(jnp.float32).astype(jnp.bfloat16)
    return jnp.where((index >= 0.0) & (index < count), index, -1.0).astype(jnp.bfloat16) == rows


def columns_of(row):
    return jnp.broadcast_to(row, (LANES, row.shape[1])).T


def thirds(values):
    first = values.astype(jnp.bfloat16).astype(jnp.float32)
    second = (values - first).astype(jnp.bfloat16).astype(jnp.float32)
    return first, second, values - first - second


AHEAD = 4


def sph_kernel(
    present_ref, pad_ref, density_ref, source_ref, carry_ref, right_ref, shift_ref, sums_ref, *scratch
):
    _, rows2, cols2, size = pad_ref.shape
    rows, cols = rows2 - 2, cols2 - 2
    tiles = rows * cols
    left_refs, exponent_refs, acc_refs = scratch[:AHEAD], scratch[AHEAD : 2 * AHEAD], scratch[2 * AHEAD :]
    x, y, vx, vy, m = [pad_ref[k] for k in range(5)]
    gx = [jnp.exp2(-LOG2E * (x + (d - 1.0)) * (x + (d - 1.0))) for d in range(3)]
    gy = [jnp.exp2(-LOG2E * (y + (d - 1.0)) * (y + (d - 1.0))) for d in range(3)]
    for di in range(3):
        for dj in range(3):
            g = gx[di] * gy[dj] * m
            carry_ref[3 * (3 * di + dj)] = g
            carry_ref[3 * (3 * di + dj) + 1] = g * vx
            carry_ref[3 * (3 * di + dj) + 2] = g * vy
    right_ref[...] = jnp.zeros_like(right_ref)
    for c, place in enumerate((x, y)):
        for n, part in enumerate(thirds((2.0 * LOG2E) * place)):
            for i in range(rows2):
                right_ref[i, :, 3 * c + n, :] = part[i]
    unit = thirds(jnp.full((1, size), 2.0 * LOG2E, jnp.float32))
    none = jnp.zeros((2, size), jnp.float32)
    for w in range(9):
        shift_ref[w] = jnp.concatenate([part * (d - 1.0) for d in (w // 3, w % 3) for part in unit] + [none], axis=0)
    sublane = lax.broadcasted_iota(jnp.int32, (8, size), 0)

    def prepare(t, slot):
        own = [thirds(pad_ref[k, t // cols + 1, pl.ds(t % cols + 1, 1), :]) for k in range(2)]
        lefts = []
        for n in range(3):
            lefts.append(
                jnp.where(sublane < 3 - n, own[0][n], jnp.where((sublane >= 3) & (sublane < 6 - n), own[1][n], 0.0))
            )
        flagged = jnp.where(sublane == 6, 1.0, lefts[0])
        left_refs[slot][...] = jnp.concatenate(lefts + [flagged] + lefts[1:], axis=0).T.astype(jnp.bfloat16)

    def expand(t, slot):
        i, j = t // cols, t % cols
        right = []
        absent = jnp.where(sublane == 6, -1024.0, 0.0)
        for w in range(9):
            near = right_ref[i + w // 3, j + w % 3]
            shift = shift_ref[w] + absent * (1.0 - present_ref[t * 9 + w])
            right.append(jnp.concatenate([near] * 3 + [shift] * 3, axis=0).astype(jnp.bfloat16))
        exponent_refs[slot][...] = jnp.dot(
            left_refs[slot][...], jnp.concatenate(right, axis=1), preferred_element_type=jnp.float32
        )

    def finish(t, slot):
        for k in range(3):
            sums_ref[k, pl.ds(t, 1), :] = jnp.sum(acc_refs[slot][k].T, axis=0, keepdims=True)

    def compute(t, slot):
        i, j = t // cols, t % cols
        half = size // 2
        for h in range(2):
            acc = [jnp.zeros((half, size), jnp.float32) for _ in range(3)]
            for w in range(9):
                weight = jnp.exp2(exponent_refs[slot][h * half : (h + 1) * half, w * size : (w + 1) * size])
                for k in range(3):
                    acc[k] = acc[k] + weight * carry_ref[3 * w + k, i + w // 3, pl.ds(j + w % 3, 1), :]
            for k in range(3):
                acc_refs[slot][k, h * half : (h + 1) * half, :] = acc[k]

    last = tiles - 1
    unroll = math.gcd(4 * AHEAD, tiles)
    for t in range(3):
        prepare(t, t)
    for t in range(2):
        expand(t, t)

    def step(p, _):
        for m in range(unroll):
            t = unroll * p + m
            n = m % AHEAD
            prepare(jnp.minimum(t + 3, last), (n + 3) % AHEAD)
            expand(jnp.minimum(t + 2, last), (n + 2) % AHEAD)
            finish(jnp.maximum(t - 1, 0), (n - 1) % AHEAD)
            compute(t, n)
        return 0

    lax.fori_loop(0, tiles // unroll, step, 0)
    finish(last, last % AHEAD)

    for i in range(rows):
        own = pad_ref[:, i + 1, 1 : cols + 1, :]
        outer = jnp.exp2(-LOG2E * (own[0] * own[0] + own[1] * own[1]))
        s0 = outer * sums_ref[0, i * cols : (i + 1) * cols, :]
        s1 = outer * sums_ref[1, i * cols : (i + 1) * cols, :]
        s2 = outer * sums_ref[2, i * cols : (i + 1) * cols, :]
        density = s0 / size
        volume = own[4] / density
        density_ref[i] = density
        source_ref[0, i * cols : (i + 1) * cols, :] = volume
        source_ref[1, i * cols : (i + 1) * cols, :] = volume * (s1 / s0)
        source_ref[2, i * cols : (i + 1) * cols, :] = volume * (s2 / s0)


def sph(padded, present):
    _, rows2, cols2, size = padded.shape
    rows, cols = rows2 - 2, cols2 - 2
    return pl.pallas_call(
        sph_kernel,
        out_shape=(
            jax.ShapeDtypeStruct((rows, cols, size), jnp.float32),
            jax.ShapeDtypeStruct((3, rows * cols, size), jnp.float32),
        ),
        in_specs=[smem(), vmem()],
        out_specs=(vmem(), vmem()),
        scratch_shapes=[
            pltpu.VMEM((27, rows2, cols2, size), jnp.float32),
            pltpu.VMEM((rows2, cols2, 8, size), jnp.float32),
            pltpu.VMEM((9, 8, size), jnp.float32),
            pltpu.VMEM((3, rows * cols, size), jnp.float32),
        ]
        + [pltpu.VMEM((size, 48), jnp.bfloat16)] * AHEAD
        + [pltpu.VMEM((size, 9 * size), jnp.float32)] * AHEAD
        + [pltpu.VMEM((3, size, size), jnp.float32)] * AHEAD,
        compiler_params=pltpu.CompilerParams(vmem_limit_bytes=VMEM_LIMIT),
        name="sph",
    )(present, padded)


def pack_kernel(source_ref, cell_ref, dest_ref, rank_ref, out_ref, acc_ref, *, group):
    tiles, size = cell_ref.shape
    devices = out_ref.shape[0]
    capacity = acc_ref.shape[1]
    acc_ref[...] = jnp.zeros_like(acc_ref)

    def work(b, _):
        lefts, rights = [], []
        for s in range(group):
            t = b * group + s
            cell = cell_ref[pl.ds(t, 1), :].astype(jnp.float32)
            upper = jnp.floor(cell * (1.0 / 256.0))
            values = [upper, cell - 256.0 * upper]
            for k in range(3):
                values.extend(split(source_ref[k, pl.ds(t, 1), :]))
            mine = is_row(dest_ref[pl.ds(t, 1), :].astype(jnp.float32), devices)
            lefts.append(
                jnp.concatenate(
                    [jnp.where(mine, value.astype(jnp.bfloat16), jnp.bfloat16(0)) for value in values], axis=0
                )
            )
            rights.append(one_hot(rank_ref[pl.ds(t, 1), :].astype(jnp.float32), capacity))
        acc_ref[...] += lax.dot_general(
            jnp.concatenate(lefts, axis=1),
            jnp.concatenate(rights, axis=1),
            (((1,), (1,)), ((), ())),
            preferred_element_type=jnp.float32,
        )
        return 0

    lax.fori_loop(0, tiles // group, work, 0)

    def part(c):
        return acc_ref[c * devices : (c + 1) * devices, :]

    outs = [256.0 * part(0) + part(1)] + [part(2 + 2 * k) + part(3 + 2 * k) for k in range(3)]
    blocks = capacity // LANES
    for k, out in enumerate(outs):
        for b in range(blocks):
            out_ref[:, k * blocks + b, :] = out[:, b * LANES : (b + 1) * LANES]


def pack(source, cell, dest, rank, devices, capacity):
    tiles, size = cell.shape
    group = math.gcd(16, tiles)
    return pl.pallas_call(
        lambda *refs: pack_kernel(*refs, group=group),
        out_shape=jax.ShapeDtypeStruct((devices, 4 * capacity // LANES, LANES), jnp.float32),
        in_specs=[vmem()] * 4,
        out_specs=vmem(),
        scratch_shapes=[pltpu.VMEM((8 * devices, capacity), jnp.float32)],
        compiler_params=pltpu.CompilerParams(vmem_limit_bytes=VMEM_LIMIT),
        name="pack",
    )(source, cell, dest, rank)


def row_and_col(cell, cells_cross):
    row = jnp.floor((cell + 0.5) * (1.0 / cells_cross))
    return row, cell - cells_cross * row


GROUP = 16
UNROLL = 3


def list_blocks(plan_ref, block_ref, *, senders, bins, blocks):
    total = 0
    together = math.gcd(8, senders)
    for q in range(bins):

        def some(g, total):
            for n in range(together):
                s = g * together + n
                first = 4 * blocks * s + plan_ref[s * bins + q]
                for b in range(blocks):
                    block_ref[total + b] = first + b
                total = total + plan_ref[(senders + s) * bins + q]
            return total

        total = lax.fori_loop(0, senders // together, some, total)
        for b in range(GROUP):
            block_ref[total + b] = -1
        total = (total + GROUP - 1) // GROUP * GROUP
        block_ref[bounds_at(senders, bins, blocks) + q] = total // GROUP
    for b in range(UNROLL * GROUP):
        block_ref[total + b] = -1


def bounds_at(senders, bins, blocks):
    return senders * (blocks + bins) + (bins + UNROLL + 1) * GROUP


def bin_of(group, bound_ref, bins):
    q = 0
    for n in range(bins - 1):
        q = q + (group >= bound_ref[n]).astype(jnp.int32)
    return q


def by_group(bound_ref, bins, work):
    def some(p, _):
        for n in range(UNROLL):
            work(UNROLL * p + n)
        return 0

    lax.fori_loop(0, (bound_ref[bins - 1] + UNROLL - 1) // UNROLL, some, 0)


def block_cells(in_ref, row, base, cells_cross):
    there = jnp.maximum(row, 0)
    row_of, col_of = row_and_col(in_ref[pl.ds(there, 1), :], cells_cross)
    return there, row_of - jnp.where(row < 0, 1 << 20, base).astype(jnp.float32), col_of


def deposit_kernel(plan_ref, in_ref, out_ref, first_ref, second_ref, block_ref, *, senders, bins, blocks):
    _, cells_along, cells_cross = out_ref.shape
    height = cells_along // bins
    list_blocks(plan_ref, block_ref, senders=senders, bins=bins, blocks=blocks)
    bound_ref = block_ref.at[pl.ds(bounds_at(senders, bins, blocks), bins)]
    out_ref[...] = jnp.zeros_like(out_ref)

    def work(group):
        base = bin_of(group, bound_ref, bins) * height
        lefts, rights = [], []
        for b in range(GROUP):
            row, row_of, col_of = block_cells(in_ref, block_ref[group * GROUP + b], base, cells_cross)
            mine = is_row(row_of, height)
            values = [part for k in range(3) for part in split(in_ref[pl.ds(row + (k + 1) * blocks, 1), :])]
            lefts.append(
                jnp.concatenate(
                    [jnp.where(mine, value.astype(jnp.bfloat16), jnp.bfloat16(0)) for value in values], axis=0
                )
            )
            rights.append(one_hot_t(col_of, cells_cross))
        both = jnp.dot(
            jnp.concatenate(lefts, axis=1), jnp.concatenate(rights, axis=0), preferred_element_type=jnp.float32
        )
        for k in range(3):
            part = both[2 * k * height : (2 * k + 1) * height] + both[(2 * k + 1) * height : (2 * k + 2) * height]
            out_ref[k, pl.ds(pl.multiple_of(base, height), height), :] += part

    by_group(bound_ref, bins, work)
    margin = first_ref.shape[1]
    even = plan_ref[2 * senders * bins] > 0
    top, bottom = out_ref[:, :margin, :], out_ref[:, cells_along - margin :, :]
    first_ref[...] = jnp.where(even, bottom, top)
    second_ref[...] = jnp.where(even, top, bottom)


def deposit(incoming, plan, bins, margin, cells_along, cells_cross):
    senders = incoming.shape[0]
    blocks = incoming.shape[1] // 4
    return pl.pallas_call(
        lambda *refs: deposit_kernel(*refs, senders=senders, bins=bins, blocks=blocks),
        out_shape=(
            jax.ShapeDtypeStruct((3, cells_along, cells_cross), jnp.float32),
            jax.ShapeDtypeStruct((3, margin, cells_cross), jnp.float32),
            jax.ShapeDtypeStruct((3, margin, cells_cross), jnp.float32),
            jax.ShapeDtypeStruct((bounds_at(senders, bins, blocks) + bins,), jnp.int32),
        ),
        in_specs=[smem(), vmem()],
        out_specs=(vmem(), vmem(), vmem(), smem()),
        compiler_params=pltpu.CompilerParams(vmem_limit_bytes=VMEM_LIMIT),
        name="deposit",
    )(plan, incoming.reshape(-1, LANES))


def substeps(edge_ref, water_ref, source_ref, state_ref, margin, *fields):
    _, cells_along, cells_cross = state_ref.shape
    _, height, width = source_ref.shape
    groups = height // 8
    slope = 0.5 * courant
    rows = lax.broadcasted_iota(jnp.int32, (8, width), 0)
    cols = lax.broadcasted_iota(jnp.int32, (8, width), 1)
    inside_cols = (cols >= edge_ref[2]) & (cols < edge_ref[3])
    nothing = [jnp.zeros((8, width), jnp.float32)] * 3

    def terms(old, g):
        at = slice(8 * g, 8 * g + 8)
        h, u, v = [old[k, at, :] for k in range(3)]
        depth = slope * water_ref[3, at, :]
        flux_x, flux_y, height_x = depth * u, depth * v, slope * h
        h, u, v = 0.25 * h, 0.25 * u, 0.25 * v
        east = [pltpu.roll(term, 7, 0) for term in (h - flux_x, u - height_x, v)]
        west = [pltpu.roll(term, 1, 0) for term in (h + flux_x, u + height_x, v)]
        north = [pltpu.roll(term, width - 1, 1) for term in (h - flux_y, u, v - height_x)]
        south = [pltpu.roll(term, 1, 1) for term in (h + flux_y, u, v + height_x)]
        return east, west, [a + b for a, b in zip(north, south)]

    old = water_ref
    for n in range(SUBSTEPS):
        new = fields[n % 2]
        before, (east, west, across) = nothing, terms(old, 0)
        for g in range(groups):
            after = terms(old, g + 1) if g + 1 < groups else (nothing, nothing, nothing)
            inside = inside_cols & (rows >= edge_ref[0] - 8 * g) & (rows < edge_ref[1] - 8 * g)
            for k in range(3):
                value = jnp.where(rows == 7, after[0][k], east[k]) + jnp.where(rows == 0, before[k], west[k])
                value = value + across[k] + source_ref[k, 8 * g : 8 * g + 8, :]
                new[k, 8 * g : 8 * g + 8, :] = jnp.where(inside, value, 0.0)
            before, (east, west, across) = west, after
        old = new
    for k in range(3):
        for first in range(0, cells_along, 8):
            block = old[k, margin + first : margin + first + 8, :]
            state_ref[k, first : first + 8, :] = pltpu.roll(block, width - margin, 1)[:, :cells_cross]


def lookup_kernel(
    block_ref, edge_ref, in_ref, water_ref, source_ref, out_ref, state_ref, left_ref, *fields, bins, blocks, margin
):
    _, cells_along, cells_cross = state_ref.shape
    height = cells_along // bins
    bound_ref = block_ref.at[pl.ds(bounds_at(in_ref.shape[0] // (4 * blocks), bins, blocks), bins)]
    substeps(edge_ref, water_ref, source_ref, state_ref, margin, *fields)
    for k in range(3):
        for h, value in enumerate(split(state_ref[k])):
            q = 2 * k + h
            for n in range(bins):
                left_ref[n, q * height : (q + 1) * height, :] = value[n * height : (n + 1) * height].astype(jnp.bfloat16)
    out_ref[...] = jnp.zeros_like(out_ref)

    def work(group):
        q = bin_of(group, bound_ref, bins)
        right = jnp.concatenate(
            [
                one_hot(block_cells(in_ref, block_ref[group * GROUP + b], 0, cells_cross)[2], cells_cross)
                for b in range(GROUP)
            ],
            axis=1,
        )
        every = jnp.dot(left_ref[q], right, preferred_element_type=jnp.float32)
        for b in range(GROUP):
            at = slice(b * LANES, (b + 1) * LANES)
            row, row_of, _ = block_cells(in_ref, block_ref[group * GROUP + b], q * height, cells_cross)
            mine = row_of == lax.broadcasted_iota(jnp.int32, (height, LANES), 0).astype(jnp.float32)
            for k in range(3):
                both = every[2 * k * height : (2 * k + 1) * height, at] + every[(2 * k + 1) * height : (2 * k + 2) * height, at]
                found = jnp.sum(jnp.where(mine, both, 0.0), axis=0, keepdims=True)
                out_ref[pl.ds(row - row // (4 * blocks) * blocks + k * blocks, 1), :] += found

    by_group(bound_ref, bins, work)


def lookup(incoming, block_list, edges, water, source, bins, margin, cells_along, cells_cross):
    senders, rows, _ = incoming.shape
    return pl.pallas_call(
        lambda *refs: lookup_kernel(*refs, bins=bins, blocks=rows // 4, margin=margin),
        out_shape=(
            jax.ShapeDtypeStruct((senders * rows // 4 * 3, LANES), jnp.float32),
            jax.ShapeDtypeStruct((3, cells_along, cells_cross), jnp.float32),
        ),
        in_specs=[smem()] * 2 + [vmem()] * 3,
        out_specs=(vmem(), vmem()),
        scratch_shapes=[pltpu.VMEM((bins, 6 * cells_along // bins, cells_cross), jnp.bfloat16)]
        + [pltpu.VMEM((3,) + water.shape[1:], jnp.float32)] * 2,
        compiler_params=pltpu.CompilerParams(vmem_limit_bytes=VMEM_LIMIT),
        name="lookup",
    )(block_list, edges, incoming.reshape(-1, LANES), water, source)


def unpack_kernel(in_ref, dest_ref, rank_ref, out_ref, left_ref, *, capacity, group):
    tiles, size = dest_ref.shape
    blocks = capacity // LANES
    devices = in_ref.shape[0] // (3 * blocks)
    for k in range(3):
        for b in range(blocks):
            for h, value in enumerate(split(in_ref[pl.ds(k * blocks + b, devices, stride=3 * blocks), :])):
                q = 2 * k + h
                left_ref[q * devices : (q + 1) * devices, b * LANES : (b + 1) * LANES] = value.astype(jnp.bfloat16)

    def step(b, _):
        right = jnp.concatenate(
            [one_hot(rank_ref[pl.ds(b * group + s, 1), :].astype(jnp.float32), capacity) for s in range(group)], axis=1
        )
        every = jnp.dot(left_ref[...], right, preferred_element_type=jnp.float32)
        for s in range(group):
            t = b * group + s
            at = slice(s * size, (s + 1) * size)
            mine = dest_ref[pl.ds(t, 1), :] == lax.broadcasted_iota(jnp.int32, (devices, size), 0)
            for k in range(3):
                both = every[2 * k * devices : (2 * k + 1) * devices, at]
                both = both + every[(2 * k + 1) * devices : (2 * k + 2) * devices, at]
                out_ref[k, pl.ds(t, 1), :] = jnp.sum(jnp.where(mine, both, 0.0), axis=0, keepdims=True)
        return 0

    lax.fori_loop(0, tiles // group, step, 0)


def unpack(returned, dest, rank, capacity):
    tiles, size = dest.shape
    devices = returned.shape[0] * LANES // (3 * capacity)
    group = math.gcd(16, tiles)
    return pl.pallas_call(
        lambda *refs: unpack_kernel(*refs, capacity=capacity, group=group),
        out_shape=jax.ShapeDtypeStruct((3, tiles, size), jnp.float32),
        in_specs=[vmem()] * 3,
        out_specs=vmem(),
        scratch_shapes=[pltpu.VMEM((6 * devices, capacity), jnp.bfloat16)],
        compiler_params=pltpu.CompilerParams(vmem_limit_bytes=VMEM_LIMIT),
        name="unpack",
    )(returned, dest, rank)


def is_even(axis):
    return lax.axis_index(axis) % 2 == 0


def swap(axis, first, second):
    count = lax.axis_size(axis)
    arrived = []
    for offset, payload in enumerate((first, second)):
        pairs = [(i, i + 1) for i in range(offset, count - 1, 2)]
        arrived.append(lax.ppermute(payload, axis, pairs + [(j, i) for i, j in pairs]))
    even = is_even(axis)
    return jnp.where(even, arrived[1], arrived[0]), jnp.where(even, arrived[0], arrived[1])


def in_order(axis, to_next, to_previous):
    even = is_even(axis)
    return jnp.where(even, to_next, to_previous), jnp.where(even, to_previous, to_next)


def padded_together(fields):
    arrays = [array for array, _, _ in fields]
    for step, axis in enumerate(("along", "cross")):
        heads, tails = [], []
        for array, (_, dims, width) in zip(arrays, fields):
            dim = dims[step]
            heads.append(lax.slice_in_dim(array, 0, width, axis=dim))
            tails.append(lax.slice_in_dim(array, array.shape[dim] - width, array.shape[dim], axis=dim))
        flat = lambda parts: jnp.concatenate([part.reshape(-1) for part in parts])
        before, after = swap(axis, *in_order(axis, flat(tails), flat(heads)))
        start, grown = 0, []
        for array, head, (_, dims, _) in zip(arrays, heads, fields):
            rims = [rim[start : start + head.size].reshape(head.shape) for rim in (before, after)]
            start += head.size
            grown.append(jnp.concatenate([rims[0], array, rims[1]], axis=dims[step]))
        arrays = grown
    return arrays


def slot_ranks(key, destination, devices, bins):
    groups, block = key.shape
    onehot = (key[:, :, None] == jnp.arange(devices * bins, dtype=jnp.int32)).astype(jnp.bfloat16)
    lower = (jnp.arange(block)[:, None] > jnp.arange(block)[None, :]).astype(jnp.bfloat16)
    earlier = jnp.einsum("ij,bjd->bid", lower, onehot, preferred_element_type=jnp.float32)
    counts = jnp.sum(onehot.astype(jnp.float32), axis=1)
    totals = jnp.sum(counts, axis=0).reshape(devices, bins)
    first = (jnp.cumsum(totals, axis=1) - totals).reshape(-1)
    before = jnp.cumsum(counts, axis=0) - counts + first
    return jnp.sum(onehot.astype(jnp.float32) * (earlier + before[:, None, :]), axis=2).astype(jnp.int32)


def shards(offsets, velocity, particle_mass, neighbours, owner_device, target_cell, surface, water_depth):
    _, tiles_along, tiles_cross, tile_size = offsets.shape
    _, cells_along, cells_cross = surface.shape
    along_count = lax.axis_size("along")
    cross_count = lax.axis_size("cross")
    devices = along_count * cross_count
    tiles = tiles_along * tiles_cross
    particles = tiles * tile_size
    capacity = -(-3 * particles // devices // LANES) * LANES
    margin = SUBSTEPS

    stacked = jnp.concatenate([offsets, velocity, particle_mass[None]], axis=0)
    water = jnp.concatenate([surface, water_depth[None]], axis=0)
    padded, wide_water = padded_together([(stacked, (1, 2), 1), (water, (1, 2), margin)])

    destination = owner_device.reshape(tiles, tile_size)
    cell = target_cell.reshape(tiles, tile_size)
    bins = max(1, min(4, LANES // devices))
    rank = slot_ranks(destination * bins + cell // (cells_along * cells_cross // bins), destination, devices, bins)
    present = jnp.any(neighbours[..., :, None] == jnp.arange(9, dtype=jnp.int32), axis=-2).astype(jnp.float32)

    density, sources = sph(padded, present.reshape(-1))
    outgoing = pack(sources, cell, destination, rank, devices, capacity)
    incoming = lax.all_to_all(outgoing, ("along", "cross"), split_axis=0, concat_axis=0, tiled=True)
    blocks = capacity // LANES
    to_bin = bins / (cells_along * cells_cross)
    lowest = jnp.floor(incoming[:, :blocks, 0] * to_bin)[..., None]
    highest = jnp.floor(jnp.max(incoming[:, :blocks], axis=2) * to_bin)[..., None]
    filled = (incoming[:, blocks : 2 * blocks, 0] != 0.0)[..., None]
    each = jnp.arange(bins, dtype=jnp.float32)
    plan = jnp.stack(
        [
            jnp.sum((filled & (highest < each)).astype(jnp.int32), axis=1),
            jnp.sum((filled & (lowest <= each) & (highest >= each)).astype(jnp.int32), axis=1),
        ]
    )
    plan = jnp.concatenate([plan.reshape(-1), is_even("along").astype(jnp.int32)[None]])
    grid_source, first, second, block_list = deposit(incoming, plan, bins, margin, cells_along, cells_cross)
    before, after = swap("along", first, second)
    tall = jnp.concatenate([before, grid_source, after], axis=1)
    before, after = swap("cross", *in_order("cross", tall[:, :, cells_cross - margin :], tall[:, :, :margin]))
    wide_source = jnp.concatenate([before, tall, after], axis=2)
    edges = []
    for axis, length in (("along", cells_along), ("cross", cells_cross)):
        place = lax.axis_index(axis)
        edges.append(jnp.where(place == 0, margin, 0))
        edges.append(jnp.where(place == lax.axis_size(axis) - 1, length + margin, length + 2 * margin))
    to_lanes = [(0, 0), (0, 0), (0, -(cells_cross + 2 * margin) % LANES)]
    looked, water_state = lookup(
        incoming,
        block_list,
        jnp.stack(edges).astype(jnp.int32),
        jnp.pad(wide_water, to_lanes),
        jnp.pad(wide_source, to_lanes),
        bins,
        margin,
        cells_along,
        cells_cross,
    )
    returned = lax.all_to_all(
        looked.reshape(devices, 3 * capacity), ("along", "cross"), split_axis=0, concat_axis=0, tiled=True
    ).reshape(looked.shape)
    feedback = unpack(returned, destination, rank, capacity)
    return water_state, density, feedback.reshape(3, tiles_along, tiles_cross, tile_size)


def solution(mesh):
    in_specs = (
        P(None, "along", "cross", None),
        P(None, "along", "cross", None),
        P("along", "cross", None),
        P("along", "cross", None),
        P("along", "cross", None, None),
        P("along", "cross", None),
        P(None, "along", "cross"),
        P("along", "cross"),
    )
    out_specs = (
        P(None, "along", "cross"),
        P("along", "cross", None),
        P(None, "along", "cross", None),
    )
    return jax.shard_map(shards, mesh=mesh, in_specs=in_specs, out_specs=out_specs, check_vma=False)
```
